64 devices in a mesh: data: 4 (over x, y), stage: 16 (over z, core).
Axes of the slice: x: 2, y: 2, z: 8, core: 2. Of those that a mesh axis runs over, the one named last changes fastest.
The devices are a block of a 4x4x8 slice.
Arguments:
- micro_in: bfloat16 [128, 128, 384], P('data'), parts along dimension 0
- targets: bfloat16 [128, 128, 384], P('data'), parts along dimension 0
- w_in: bfloat16 [16, 2, 384, 1536], P('stage')
- w_out: bfloat16 [16, 2, 1536, 384], P('stage')
Outputs:
- output 1: float32 [64, 2, 384, 1536], P(('data', 'stage')), parts along dimension 0
- output 2: float32 [64, 2, 1536, 384], P(('data', 'stage')), parts along dimension 0
- output 3: float32 [4], P('data'), parts along dimension 0
There are 4 independent parts. The reference program is written for one: setup_inputs(seed, part) draws one part's arguments, and reference() takes and returns one part's arrays. A program takes and returns all parts, laid end to end along the dimension named above; an argument that names none is the same for every part.
All inputs are finite; a program needn't handle non-finite values.
Results may differ from the reference program's by a relative error of at most 0.00438966.
Values are sent between devices in bfloat16 or wider.
A program may use at most 768 MiB of HBM per device.

```python
import jax
import jax.numpy as jnp
from jax import lax

STAGES = 16
MICRO = 32
TOKENS = 128
D = 384
FF = 1536


def setup_inputs(seed: int = 0, part: int = 0) -> dict:
    part_key = jax.random.fold_in(jax.random.key(seed), part)
    key_x, key_t = jax.random.split(part_key)
    key_a, key_b = jax.random.split(jax.random.key(seed + 1))
    micro_in = jax.random.normal(key_x, (MICRO, TOKENS, D), jnp.float32)
    targets = jax.random.normal(key_t, (MICRO, TOKENS, D), jnp.float32)
    w_in = jax.random.normal(key_a, (STAGES, 2, D, FF), jnp.float32) * D ** -0.5
    w_out = jax.random.normal(key_b, (STAGES, 2, FF, D), jnp.float32) * (2.0 / (FF * STAGES)) ** 0.5
    return {'micro_in': micro_in.astype(jnp.bfloat16), 'targets': targets.astype(jnp.bfloat16), 'w_in': w_in.astype(jnp.bfloat16), 'w_out': w_out.astype(jnp.bfloat16)}


def gelu_pair(pre_f32):
    gelu_val, pull_fn = jax.vjp(jax.nn.gelu, pre_f32)
    return gelu_val, pull_fn(jnp.ones_like(pre_f32))[0]


def reference(micro_in, targets, w_in, w_out):
    layer_count = 2 * STAGES
    w_first = w_in.reshape(layer_count, D, FF)
    w_second = w_out.reshape(layer_count, FF, D)
    loss_scale = 1.0 / (MICRO * TOKENS * D)

    def layer_fwd(h_cur, weights):
        w_a, w_b = weights
        pre_act = jnp.dot(h_cur, w_a, preferred_element_type=jnp.float32).astype(jnp.bfloat16)
        act_val = jax.nn.gelu(pre_act.astype(jnp.float32)).astype(jnp.bfloat16)
        branch = jnp.dot(act_val, w_b, preferred_element_type=jnp.float32)
        return (h_cur.astype(jnp.float32) + branch).astype(jnp.bfloat16), (h_cur, pre_act)

    def layer_bwd(grad_h, layer_items):
        w_a, w_b, h_cur, pre_act = layer_items
        act_f32, gelu_slope = gelu_pair(pre_act.astype(jnp.float32))
        act_val = act_f32.astype(jnp.bfloat16)
        grad_act = jnp.dot(grad_h, w_b.T, preferred_element_type=jnp.float32)
        grad_pre = (gelu_slope * grad_act).astype(jnp.bfloat16)
        back_sum = jnp.dot(grad_pre, w_a.T, preferred_element_type=jnp.float32)
        grad_in = (grad_h.astype(jnp.float32) + back_sum).astype(jnp.bfloat16)
        grad_wa = jnp.dot(h_cur.T, grad_pre, preferred_element_type=jnp.float32)
        grad_wb = jnp.dot(act_val.T, grad_h, preferred_element_type=jnp.float32)
        return grad_in, (grad_wa, grad_wb)

    def one_micro(carry_state, micro_pair):
        acc_a, acc_b, loss_acc = carry_state
        x_now, tgt_now = micro_pair
        y_out, saved_acts = lax.scan(layer_fwd, x_now, (w_first, w_second))
        residual = y_out.astype(jnp.float32) - tgt_now.astype(jnp.float32)
        loss_acc = loss_acc + 0.5 * jnp.sum(residual * residual) * loss_scale
        grad_top = (residual * loss_scale).astype(jnp.bfloat16)
        grad_pair = lax.scan(layer_bwd, grad_top, (w_first, w_second, saved_acts[0], saved_acts[1]), reverse=True)[1]
        return (acc_a + grad_pair[0], acc_b + grad_pair[1], loss_acc), None

    init_state = (jnp.zeros((layer_count, D, FF), jnp.float32), jnp.zeros((layer_count, FF, D), jnp.float32), jnp.zeros((), jnp.float32))
    final_state = lax.scan(one_micro, init_state, (micro_in, targets))[0]
    acc_a, acc_b, loss_acc = final_state
    return acc_a.reshape(STAGES, 2, D, FF), acc_b.reshape(STAGES, 2, FF, D), loss_acc.reshape(1)
```

```python
import functools

import jax
import jax.numpy as jnp
import numpy as np
from jax import lax
from jax.experimental import pallas as pl
from jax.experimental.pallas import tpu as pltpu
from jax.sharding import PartitionSpec as P

BF16 = jnp.bfloat16
F32 = jnp.float32
C0 = float(np.sqrt(2.0 / np.pi))
C1 = C0 * 0.044715
TILE = 256
LAG = 2


def dot(x, w):
    return jnp.dot(x, w, preferred_element_type=F32)


def gelu(u):
    t = jnp.tanh(u * (C0 + C1 * (u * u)))
    return u * (0.5 * t + 0.5)


def gelu_slope(u_bf):
    u = jnp.clip(u_bf, -1024.0, 1024.0).astype(F32)
    u2 = u * u
    t = jnp.tanh(u * (C0 + C1 * u2))
    w = u * (0.5 * C0 + (1.5 * C1) * u2)
    return (1.0 + t) * (0.5 + (1.0 - t) * w)


def layer(x, w1, w2, tiles, middle):
    acc = None
    mids = []
    for n in range(tiles + LAG):
        if n < tiles:
            mids.append(middle(n, dot(x, w1[:, n * TILE:(n + 1) * TILE])))
        if n >= LAG:
            k = n - LAG
            part = dot(mids[k], w2[k * TILE:(k + 1) * TILE, :])
            acc = part if acc is None else acc + part
    return (x.astype(F32) + acc).astype(BF16)


def pipeline_kernel(stages, x_hbm, t_hbm, wi_hbm, wo_hbm, sh, sa, se, sg, loss_ref, wa, wb, wat, wbt, hin, gin, us, ast, hst,
                    est, gst, hsend, gsend, lacc, lpeer, lrecv, wa_sem, wb_sem, wsend_sem, fin_sem, gin_sem, hs_sem, gs_sem,
                    fa_sem, fh_sem, be_sem, bg_sem, stash_sem, lp_sem, lr_sem):
    k = lax.axis_index('stage')
    chips = stages // 2
    s = k // 2
    c = k % 2
    last = chips - 1
    peer = k + 1 - 2 * c
    num_micro, tokens, dim = x_hbm.shape
    hidden = wi_hbm.shape[-1]
    own = wi_hbm.shape[0]
    layers = 2 * own
    nb = num_micro // 2
    tiles = hidden // TILE
    scale = 1.0 / (num_micro * tokens * dim)

    def dev(idx):
        return {'stage': idx}

    def copy(src, dst, sem):
        return pltpu.make_async_copy(src, dst, sem)

    def remote(src, dst, send, recv, idx):
        return pltpu.make_async_remote_copy(src_ref=src, dst_ref=dst, send_sem=send, recv_sem=recv, device_id=dev(idx),
                                            device_id_type=pl.DeviceIdType.MESH)

    for ll in range(own):
        copy(wi_hbm.at[ll], wa.at[own * c + ll], wa_sem.at[own * c + ll]).start()
        copy(wo_hbm.at[ll], wb.at[own * c + ll], wb_sem.at[own * c + ll]).start()

    @pl.when(s == 0)
    def _():
        @pl.loop(0, nb)
        def _(i):
            copy(x_hbm.at[c * nb + i], hin.at[i], fin_sem.at[i]).start()

    @pl.when(s == last)
    def _():
        @pl.loop(0, nb)
        def _(i):
            copy(t_hbm.at[c * nb + i], gin.at[i], gin_sem.at[i]).start()

    barrier = pltpu.get_barrier_semaphore()
    pl.semaphore_signal(barrier, inc=1, device_id=dev(peer), device_id_type=pl.DeviceIdType.MESH)

    @pl.when(s > 0)
    def _():
        pl.semaphore_signal(barrier, inc=1, device_id=dev(k - 2), device_id_type=pl.DeviceIdType.MESH)

    @pl.when(s < last)
    def _():
        pl.semaphore_signal(barrier, inc=1, device_id=dev(k + 2), device_id_type=pl.DeviceIdType.MESH)

    pl.semaphore_wait(barrier, 1 + jnp.where(s > 0, 1, 0) + jnp.where(s < last, 1, 0))

    def weight_sends():
        out = []
        for ll in range(own):
            l = own * c + ll
            out.append(remote(wi_hbm.at[ll], wa.at[l], wsend_sem.at[2 * ll], wa_sem.at[l], peer))
            out.append(remote(wo_hbm.at[ll], wb.at[l], wsend_sem.at[2 * ll + 1], wb_sem.at[l], peer))
        return out

    for send in weight_sends():
        send.start()
    lacc[...] = jnp.zeros_like(lacc)
    for l in range(layers):
        copy(wa.at[l], wa.at[l], wa_sem.at[l]).wait()
        copy(wb.at[l], wb.at[l], wb_sem.at[l]).wait()

    def transposes():
        @pl.loop(0, layers * tiles)
        def _(j):
            l = j // tiles
            at = pl.ds(pl.multiple_of((j % tiles) * TILE, TILE), TILE)
            wat[l, at, :] = wa[l, :, at].T
            wbt[l, :, at] = wb[l, at, :].T

    warm = jnp.minimum(nb, 1 + (13 * (last - s) + 4) // 5)

    @pl.when(s > 0)
    def _():
        transposes()

    def stash_forward(i, par):
        for l in range(layers):
            ll = l % own
            a_at, h_at = ast.at[par, l], (hin.at[i] if l == 0 else hst.at[par, l - 1])
            yield l // own, (a_at, sa.at[ll, c, i], fa_sem.at[par, l], stash_sem.at[1, ll]), (h_at, sh.at[ll, c, i], fh_sem.at[par, l], stash_sem.at[0, ll])

    def stash_backward(i, par):
        for l in range(layers):
            ll = l % own
            e_at, g_at = est.at[par, l], (gin.at[i] if l == layers - 1 else gst.at[par, l])
            yield l // own, (e_at, se.at[ll, c, i], be_sem.at[par, l], stash_sem.at[2, ll]), (g_at, sg.at[ll, c, i], bg_sem.at[par, l], stash_sem.at[3, ll])

    def stash_start(pairs):
        for owner, one, two in pairs:
            @pl.when(c == owner)
            def _():
                copy(*one[:3]).start()
                copy(*two[:3]).start()

            @pl.when(c != owner)
            def _():
                remote(*one, peer).start()
                remote(*two, peer).start()

    def stash_wait(pairs):
        for owner, one, two in pairs:
            @pl.when(c == owner)
            def _():
                copy(*one[:3]).wait()
                copy(*two[:3]).wait()

            @pl.when(c != owner)
            def _():
                remote(*one, peer).wait_send()
                remote(*two, peer).wait_send()

    def h_send(i, par):
        return remote(hsend.at[par], hin.at[i], hs_sem.at[par], fin_sem.at[i], k + 2)

    def g_send(i, par):
        return remote(gsend.at[par], gin.at[i], gs_sem.at[par], gin_sem.at[i], k - 2)

    def forward(i):
        par = i % 2

        @pl.when(i >= 2)
        def _():
            stash_wait(stash_forward(i - 2, par))

            @pl.when(s < last)
            def _():
                h_send(i - 2, par).wait_send()

        copy(hin.at[i], hin.at[i], fin_sem.at[i]).wait()
        x = hin[i]
        for l in range(layers):
            if l > 0:
                hst[par, l - 1] = x

            def middle(n, p, l=l):
                at = slice(n * TILE, (n + 1) * TILE)
                u = p.astype(BF16)
                us[i, l, :, at] = u
                a = gelu(u.astype(F32)).astype(BF16)
                ast[par, l, :, at] = a
                return a

            x = layer(x, wa.at[l], wb.at[l], tiles, middle)
        hsend[par] = x

        @pl.when(s < last)
        def _():
            h_send(i, par).start()

        stash_start(stash_forward(i, par))

        @pl.when(s == last)
        def _():
            copy(gin.at[i], gin.at[i], gin_sem.at[i]).wait()
            r = hsend[par].astype(F32) - gin[i].astype(F32)
            gin[i] = (r * scale).astype(BF16)
            lacc[...] += jnp.sum((r * r).reshape(tokens // 8, 8, dim), axis=0)

            @pl.when(i == nb - 1)
            def _():
                remote(lacc, lpeer, lp_sem.at[0], lp_sem.at[1], peer).start()

    def backward(i):
        par = i % 2

        @pl.when(i >= 2)
        def _():
            stash_wait(stash_backward(i - 2, par))

            @pl.when(s > 0)
            def _():
                g_send(i - 2, par).wait_send()

        @pl.when(s < last)
        def _():
            copy(gin.at[i], gin.at[i], gin_sem.at[i]).wait()

        g = gin[i]
        for l in reversed(range(layers)):
            if l < layers - 1:
                gst[par, l] = g

            def middle(n, p, l=l):
                at = slice(n * TILE, (n + 1) * TILE)
                e = (gelu_slope(us[i, l, :, at]) * p).astype(BF16)
                est[par, l, :, at] = e
                return e

            g = layer(g, wbt.at[l], wat.at[l], tiles, middle)
        gsend[par] = g

        @pl.when(s > 0)
        def _():
            g_send(i, par).start()

        stash_start(stash_backward(i, par))

        @pl.when(i == nb - 1)
        def _():
            @pl.when(s == last)
            def _():
                remote(lacc, lpeer, lp_sem.at[0], lp_sem.at[1], peer).wait()
                lrecv[...] = jnp.full(lrecv.shape, jnp.sum(lacc[...] + lpeer[...]) * (0.5 * scale), F32)

            @pl.when(s < last)
            def _():
                copy(lrecv, lrecv, lr_sem.at[1]).wait()

            loss_ref[...] = lrecv[...]

            @pl.when(s > 0)
            def _():
                send = remote(lrecv, lrecv, lr_sem.at[0], lr_sem.at[1], k - 2)
                send.start()
                send.wait_send()

    @pl.loop(0, nb + warm)
    def _(j):
        @pl.when((j == warm) & (s == 0))
        def _():
            transposes()

        @pl.when(j >= warm)
        def _():
            backward(j - warm)

        @pl.when(j < nb)
        def _():
            forward(j)

    for send in weight_sends():
        send.wait_send()
    for i in (nb - 2, nb - 1):
        stash_wait(stash_forward(i, i % 2))
        stash_wait(stash_backward(i, i % 2))

        @pl.when(s < last)
        def _():
            h_send(i, i % 2).wait_send()

        @pl.when(s > 0)
        def _():
            g_send(i, i % 2).wait_send()

    for ll in range(own):
        for kind, ref in enumerate((sh, sa, se, sg)):
            there = ref.at[ll, 1 - c]
            copy(there, there, stash_sem.at[kind, ll]).wait()


def solution(mesh):
    stages = mesh.shape['stage']

    def per_device(micro_in, targets, w_in, w_out):
        num_micro, tokens, dim = micro_in.shape
        own, hidden = w_in.shape[1], w_in.shape[3]
        layers = 2 * own
        nb = num_micro // 2
        hbm = pl.BlockSpec(memory_space=pl.ANY)
        vm = pltpu.VMEM
        dma = pltpu.SemaphoreType.DMA
        wide = jax.ShapeDtypeStruct((own, 2, nb, tokens, hidden), BF16)
        narrow = jax.ShapeDtypeStruct((own, 2, nb, tokens, dim), BF16)
        sh, sa, se, sg, loss = pl.pallas_call(
            functools.partial(pipeline_kernel, stages),
            out_shape=(narrow, wide, wide, narrow, jax.ShapeDtypeStruct((8, 128), F32)),
            in_specs=[hbm] * 4,
            out_specs=(hbm, hbm, hbm, hbm, pl.BlockSpec(memory_space=pltpu.VMEM)),
            scratch_shapes=[
                vm((layers, dim, hidden), BF16), vm((layers, hidden, dim), BF16),
                vm((layers, hidden, dim), BF16), vm((layers, dim, hidden), BF16),
                vm((nb, tokens, dim), BF16), vm((nb, tokens, dim), BF16),
                vm((nb, layers, tokens, hidden), BF16),
                vm((2, layers, tokens, hidden), BF16), vm((2, layers - 1, tokens, dim), BF16),
                vm((2, layers, tokens, hidden), BF16), vm((2, layers - 1, tokens, dim), BF16),
                vm((2, tokens, dim), BF16), vm((2, tokens, dim), BF16),
                vm((8, dim), F32), vm((8, dim), F32), vm((8, 128), F32),
                dma((layers,)), dma((layers,)), dma((2 * own,)), dma((nb,)), dma((nb,)), dma((2,)), dma((2,)),
                dma((2, layers)), dma((2, layers)), dma((2, layers)), dma((2, layers)), dma((4, own)), dma((2,)), dma((2,)),
            ],
            compiler_params=pltpu.CompilerParams(collective_id=0, has_side_effects=True, vmem_limit_bytes=67043328),
            name='pipeline',
        )(micro_in, targets, w_in[0], w_out[0])

        def grad(left, right):
            left = left.reshape(own, num_micro * tokens, left.shape[-1])
            right = right.reshape(own, num_micro * tokens, right.shape[-1])
            return jnp.einsum('lti,ltj->lij', left, right, preferred_element_type=F32)

        return grad(sh, se)[None], grad(sa, sg)[None], loss[0, :1]

    return jax.shard_map(per_device, mesh=mesh, in_specs=(P('data'), P('data'), P('stage'), P('stage')),
                         out_specs=(P(('data', 'stage')), P(('data', 'stage')), P('data')), check_vma=False)
```
